256 devices in a mesh: group: 2 (over y), station: 16 (over z), tm: 4 (over x), chan: 2 (over core).
Axes of the slice: x: 4, y: 2, z: 16, core: 2. Of those that a mesh axis runs over, the one named last changes fastest.
The devices are a block of a 4x16x16 slice.
Arguments:
- voltages: bfloat16 [32, 128, 2, 96, 512], P(('group', 'station'), 'chan', None, None, 'tm'), parts along dimension 0, may hold values from -6 to 6
- delays: int32 [32], P(('group', 'station')), parts along dimension 0, may hold values from 0 to 16, as said below
- tap_sets: int32 [32, 128], P(('group', 'station'), 'chan'), parts along dimension 0, may hold values from 0 to 15
- tap_table: bfloat16 [16, 16], replicated, may hold values from -1.5 to 1.5
- weights: bfloat16 [32, 128, 2, 96, 128], P(('group', 'station'), 'chan'), parts along dimension 0, may hold values from -0.15625 to 0.15625
Outputs:
- array_beams: bfloat16 [256, 2, 128, 512], P(('group', 'chan', 'station'), None, None, 'tm'), parts along dimension 0
The draws below stay inside these ranges and needn't reach their ends.
There are 2 independent parts, one for each index of `group`. The reference program is written for one: setup_inputs(seed, part) draws one part's arguments, and reference() takes and returns one part's arrays. A program takes and returns all parts, laid end to end along the dimension named above; an argument that names none is the same for every part. Nothing has to cross between parts.
Inputs may be any that keep to these rules, and one draw needn't show every extreme that they name: `delays`: every delay lies in 0 to 16, and some station has delay 16.
All inputs are finite; a program needn't handle non-finite values.
Results may differ from the reference program's by a relative error of at most 0.0049.
Values may be sent and summed in bfloat16 or wider, within the bound.
No kernel may reach another device: no remote copies, remote signals or barrier semaphores. Data moves between devices by JAX's collectives and lax.ppermute only.
A program may use at most 64 MiB of HBM per device.

```python
import jax
import jax.numpy as jnp
from jax import lax

ANTENNA_COUNT = 96
BEAM_TOTAL = 128
TAPS = 16
MAXD = 16
NSETS = 16
STATION_TOTAL = 16
FREQUENCY_BINS = 128
TIME_SAMPLES = 512


def draw_delays(key, part):
    drawn = jax.random.randint(key, (STATION_TOTAL,), 0, MAXD + 1)
    chosen = jax.random.randint(jax.random.fold_in(key, 7), (), 0, STATION_TOTAL)
    positions = jnp.arange(STATION_TOTAL)
    return jnp.where(positions == chosen, MAXD, drawn).astype(jnp.int32)


def plant(array, own_key, least, largest):
    longest = array.shape.index(max(array.shape))
    spots = []
    for shift in (0, 1):
        where = [jax.random.randint(jax.random.fold_in(own_key, axis), (), 0, length) for axis, length in enumerate(array.shape)]
        where[longest] = (where[longest] + shift) % array.shape[longest]
        spots.append(tuple(where))
    return array.at[spots[0]].set(least).at[spots[1]].set(largest)


def raised(values, key, source, target, shards_of, factor):
    def block_of(axis_at):
        return (jnp.arange(values.shape[axis_at]) // (values.shape[axis_at] // shards_of)).reshape((-1,) + (1,) * (values.ndim - 1 - axis_at))

    near = jax.random.permutation(key, shards_of)[block_of(target)]
    other_side = (block_of(target) + shards_of // 2) % shards_of
    return jnp.where((block_of(source) == near) | (block_of(source) == other_side), factor * values, values)


def levels(key, dims, cuts, low, top_value):
    def one(dim, parts):
        heights = jax.random.uniform(jax.random.fold_in(jax.random.fold_in(key, 6), dim), (parts,), jnp.float32, low / len(cuts), top_value / len(cuts))
        return jnp.repeat(jnp.exp(heights), dims[dim] // parts).reshape((-1,) + (1,) * (len(dims) - dim - 1))

    level = one(*cuts[0])
    for cut in cuts[1:]:
        level = level * one(*cut)
    return level


def gaussian(own_key, dims, width, reach, pieces=(), dtype=jnp.bfloat16):
    loudness = levels(own_key, dims, pieces, -0.22, 0.18) if pieces else 1.0
    array = jax.random.normal(own_key, dims, jnp.float32) * width * loudness
    return jnp.minimum(jnp.maximum(array, -reach), reach).astype(dtype)


def bell_draw_with(key, shape, spread, reach, split, heavy, held_as=jnp.bfloat16):
    values = spread * jax.random.normal(key, shape, jnp.float32)
    if split:
        values = values * levels(key, shape, split, -0.22, 0.18)
    return jnp.clip(raised(values, jax.random.fold_in(key, 3), *heavy), -reach, reach).astype(held_as)


def setup_inputs(seed: int = 0, part: int = 0) -> dict:
    key_of = jax.random.split(jax.random.key(seed), 6)
    part_splits = jax.random.split(jax.random.fold_in(key_of[5], part), 6)
    voltages = gaussian(part_splits[0], (STATION_TOTAL, FREQUENCY_BINS, 2, ANTENNA_COUNT, TIME_SAMPLES), 1.0, 6.0, ((0, 16), (1, 2), (4, 4)))
    delays = draw_delays(jax.random.fold_in(jax.random.fold_in(key_of[5], part), 71), part)
    tap_sets = plant(jax.random.randint(part_splits[2], (STATION_TOTAL, FREQUENCY_BINS), 0, NSETS), jax.random.fold_in(part_splits[2], 1), 0, NSETS - 1).astype(jnp.int32)
    tap_table = gaussian(key_of[3], (NSETS, TAPS), 0.25, 1.5)
    weights = bell_draw_with(part_splits[4], (STATION_TOTAL, FREQUENCY_BINS, 2, ANTENNA_COUNT, BEAM_TOTAL), (2 * ANTENNA_COUNT * STATION_TOTAL) ** -0.5, 0.15625, ((0, 16), (1, 2)), (0, 1, 16, 2.0))
    return {"voltages": voltages, "delays": delays, "tap_sets": tap_sets, "tap_table": tap_table, "weights": weights}


def reference(voltages, delays, tap_sets, tap_table, weights):
    halo_len = MAXD + TAPS - 1
    table_f32 = tap_table.astype(jnp.float32)

    def one_station(running, station_item):
        samples, delay_now, chosen_sets, steer = station_item
        samples_f32 = samples.astype(jnp.float32)
        padded = jnp.pad(samples_f32, ((0, 0), (0, 0), (0, 0), (halo_len, 0)))
        coefficients = table_f32[chosen_sets]
        summed_taps = jnp.zeros(samples_f32.shape, jnp.float32)
        for tap_index in range(TAPS):
            begin = (halo_len - delay_now - tap_index).astype(jnp.int32)
            shifted = lax.dynamic_slice_in_dim(padded, begin, TIME_SAMPLES, 3)
            summed_taps = summed_taps + coefficients[:, tap_index][:, None, None, None] * shifted
        delayed_voltages = lax.optimization_barrier(summed_taps.astype(jnp.bfloat16)).astype(jnp.float32)
        steer_f32 = steer.astype(jnp.float32)
        real_in = delayed_voltages[:, 0]
        imag_in = delayed_voltages[:, 1]
        real_part = jnp.einsum('cat,cab->cbt', real_in, steer_f32[:, 0]) - jnp.einsum('cat,cab->cbt', imag_in, steer_f32[:, 1])
        imag_part = jnp.einsum('cat,cab->cbt', real_in, steer_f32[:, 1]) + jnp.einsum('cat,cab->cbt', imag_in, steer_f32[:, 0])
        return running + jnp.stack([real_part, imag_part], axis=1), None

    start_sum = jnp.zeros((FREQUENCY_BINS, 2, BEAM_TOTAL, TIME_SAMPLES), jnp.float32)
    result, unused = lax.scan(one_station, start_sum, (voltages, delays, tap_sets, weights))
    return result.astype(jnp.bfloat16)
```

```python
import functools

import jax
import jax.numpy as jnp
from jax import lax
from jax.experimental import pallas as pl
from jax.experimental.pallas import tpu as pltpu
from jax.sharding import PartitionSpec as P


TAPS = 16
HALO = 32


ANY = pl.BlockSpec(memory_space=pl.ANY)
VMEM = pl.BlockSpec(memory_space=pltpu.VMEM)
SMEM = pl.BlockSpec(memory_space=pltpu.SMEM)
PARAMS = pltpu.CompilerParams(vmem_limit_bytes=16 * 1024 * 1024)


def near(value, space=pltpu.VMEM):
    return pltpu.with_memory_space_constraint(value, space)


def passed_along(value, axis, step, wrap):
    count = lax.axis_size(axis)
    pairs = [(source, (source + step) % count) for source in range(count)]
    if not wrap:
        pairs = [(source, target) for source, target in pairs if target == source + step]
    return lax.ppermute(value, axis, pairs)


def chunk_index(offset, count):
    return lax.rem(lax.axis_index("station") + (offset % count), count)


def pack_near_kernel(offsets, count, x_ref, packed_ref):
    rows, _, length = x_ref.shape[1:]
    for i, offset in enumerate(offsets):
        chunk = chunk_index(offset, count)
        packed_ref[i] = jnp.concatenate(
            [x_ref[chunk, q, :, length - HALO :] for q in range(rows)], axis=-1
        )


def pack_kernel(offsets, count, x_ref, packed_ref, buf, sem):
    copies = [
        pltpu.make_async_copy(x_ref.at[chunk_index(offset, count)], buf.at[i], sem.at[i])
        for i, offset in enumerate(offsets)
    ]
    for copy in copies:
        copy.start()
    rows = buf.shape[1]
    length = buf.shape[-1]
    for i, copy in enumerate(copies):
        copy.wait()
        packed_ref[i] = jnp.concatenate(
            [buf[i, q, :, length - HALO :] for q in range(rows)], axis=-1
        )


def pack(x, offsets, direct):
    count, rows, height, length = x.shape
    shape = pltpu.VMEM((len(offsets), height, rows * HALO), x.dtype)
    if direct:
        return pl.pallas_call(
            functools.partial(pack_near_kernel, offsets, count),
            out_shape=shape,
            in_specs=[VMEM],
            out_specs=VMEM,
            compiler_params=PARAMS,
            name="pack",
        )(near(x))
    return pl.pallas_call(
        functools.partial(pack_kernel, offsets, count),
        out_shape=shape,
        in_specs=[ANY],
        out_specs=VMEM,
        scratch_shapes=[
            pltpu.VMEM((len(offsets), rows, height, length), x.dtype),
            pltpu.SemaphoreType.DMA((len(offsets),)),
        ],
        compiler_params=PARAMS,
        name="pack",
    )(near(x, pltpu.HBM))


def bank_kernel(table_ref, delay_ref, x_ref, w_ref, main_ref, halo_ref, near_x_ref, near_w_ref, sem):
    sets, length, _ = main_ref.shape
    delay = delay_ref[0]
    block = 16
    copies = [
        pltpu.make_async_copy(x_ref, near_x_ref, sem.at[0]),
        pltpu.make_async_copy(w_ref, near_w_ref, sem.at[1]),
    ]
    for copy in copies:
        copy.start()

    def fill(ref, start, shift):
        row = lax.broadcasted_iota(jnp.int32, (block, ref.shape[-1]), 0) + start
        lane = lax.broadcasted_iota(jnp.int32, (block, ref.shape[-1]), 1)
        lag = row - delay + shift(lane)
        rows = [jnp.zeros(lag.shape, jnp.float32) for _ in range(sets)]
        for k in range(TAPS):
            hit = lag == k
            for m in range(sets):
                rows[m] = jnp.where(hit, table_ref[m, k], rows[m])
        for m in range(sets):
            ref[m, pl.ds(start, block), :] = rows[m].astype(ref.dtype)

    @pl.loop(0, length // block)
    def _(i):
        fill(main_ref, pl.multiple_of(i * block, block), lambda lane: -lane)

    @pl.loop(0, HALO // block)
    def _(i):
        fill(halo_ref, pl.multiple_of(i * block, block), lambda lane: HALO - lax.rem(lane, HALO))

    for copy in copies:
        copy.wait()


def bank(table, delays, x, w):
    length = x.shape[-1]
    sets = table.shape[0]
    return pl.pallas_call(
        bank_kernel,
        out_shape=(
            pltpu.VMEM((sets, length, length), jnp.bfloat16),
            pltpu.VMEM((sets, HALO, length), jnp.bfloat16),
            pltpu.VMEM(x.shape, x.dtype),
            pltpu.VMEM(w.shape, w.dtype),
        ),
        in_specs=[SMEM, SMEM, ANY, ANY],
        out_specs=(VMEM,) * 4,
        scratch_shapes=[pltpu.SemaphoreType.DMA((2,))],
        compiler_params=PARAMS,
        name="bank",
    )(near(table.astype(jnp.float32), pltpu.SMEM), near(delays, pltpu.SMEM), near(x, pltpu.HBM), near(w, pltpu.HBM))


def beam_kernel(parts, count, sets_ref, x_ref, w_ref, main_ref, edge_ref, halo_ref, *outs):
    _, rows, _, length = x_ref.shape
    lane_block = lax.broadcasted_iota(jnp.int32, (HALO, length), 1) // HALO
    nt = (((1,), (1,)), ((), ()))
    for offset, place, where in parts:
        chunk = chunk_index(offset, count)
        chosen = [sets_ref[0, chunk * rows + q] for q in range(rows)]
        edge = jnp.concatenate(
            [
                jnp.where(lane_block == q, edge_ref[chosen[q]], jnp.zeros((), jnp.bfloat16))
                for q in range(rows)
            ],
            axis=0,
        )
        early = lax.dot_general(edge, halo_ref[place], nt, preferred_element_type=jnp.float32)
        for q in range(rows):
            late = lax.dot_general(
                main_ref[chosen[q]], x_ref[chunk, q], nt, preferred_element_type=jnp.float32
            )
            delayed = jnp.concatenate(
                [late[:HALO] + early[q * HALO : (q + 1) * HALO], late[HALO:]], axis=0
            ).astype(jnp.bfloat16)
            real_w = w_ref[chunk, q, 0]
            imag_w = w_ref[chunk, q, 1]
            steer = jnp.concatenate(
                [
                    jnp.concatenate([real_w, imag_w], axis=-1),
                    jnp.concatenate([-imag_w, real_w], axis=-1),
                ],
                axis=0,
            )
            beams = jnp.dot(delayed, steer, preferred_element_type=jnp.float32)
            out, spot = where[q]
            outs[out][spot] = beams.astype(outs[out].dtype)


def beams_of(parts, out_rows, dtype, tap_sets, x, w, banks, halo):
    count, rows, height, length = x.shape
    beam_count = w.shape[-1]
    n_out = max(where[0] for part in parts for where in part[2]) + 1
    return pl.pallas_call(
        functools.partial(beam_kernel, parts, count),
        out_shape=(pltpu.VMEM((out_rows, length, 2 * beam_count), dtype),) * n_out,
        in_specs=[SMEM] + [VMEM] * 5,
        out_specs=(VMEM,) * n_out,
        cost_estimate=pl.CostEstimate(
            flops=len(parts) * rows * 2 * length * height * (length + 2 * beam_count),
            bytes_accessed=len(parts) * rows * height * (length + beam_count) * 2,
            transcendentals=0,
        ),
        compiler_params=PARAMS,
        name="beams",
    )(near(tap_sets, pltpu.SMEM), near(x), near(w), near(banks[0]), near(banks[1]), near(halo))


def join_kernel(right_ref, left_ref, own_right_ref, own_left_ref, to_right_ref, to_left_ref):
    split = right_ref.shape[0]
    whole = own_right_ref.shape[0]
    for q in range(whole):
        value = own_right_ref[q]
        if q < split:
            value = value + right_ref[q].astype(jnp.float32)
        to_right_ref[q] = value.astype(to_right_ref.dtype)
        value = own_left_ref[q]
        if q >= whole - left_ref.shape[0]:
            value = value + left_ref[q - whole + left_ref.shape[0]].astype(jnp.float32)
        to_left_ref[q] = value.astype(to_left_ref.dtype)


def join(right, left, own_right, own_left):
    shape = pltpu.VMEM(own_right.shape, right.dtype)
    return pl.pallas_call(
        join_kernel,
        out_shape=(shape, shape),
        in_specs=[VMEM] * 4,
        out_specs=(VMEM, VMEM),
        compiler_params=PARAMS,
        name="join",
    )(near(right), near(left), near(own_right), near(own_left))


def finish_kernel(right_ref, left_ref, own_ref, out_ref):
    rows, _, width = own_ref.shape
    half = width // 2
    for q in range(rows):
        total = (
            right_ref[q].astype(jnp.float32) + left_ref[q].astype(jnp.float32) + own_ref[q]
        )
        for part in range(2):
            out_ref[q, part] = total[:, part * half : (part + 1) * half].T.astype(out_ref.dtype)


def finish(right, left, own):
    rows, length, width = own.shape
    return pl.pallas_call(
        finish_kernel,
        out_shape=jax.ShapeDtypeStruct((rows, 2, width // 2, length), jnp.bfloat16),
        in_specs=[VMEM] * 3,
        out_specs=VMEM,
        compiler_params=PARAMS,
        name="finish",
    )(near(right), near(left), near(own))


def ring(voltages, delays, tap_sets, tap_table, weights):
    _, channels, pair, antennas, length = voltages.shape
    beam_count = weights.shape[-1]
    count = lax.axis_size("station")
    rows = channels // count
    half = count // 2
    split = rows // 2
    x = voltages.reshape(count, rows, pair * antennas, length)
    w = weights.reshape(count, rows, pair, antennas, beam_count)

    def around(s):
        return [half - s, s - half]

    pieces = [[half] + around(1)]
    pieces.append([o for s in range(2, 5) for o in around(s)])
    pieces.append([o for s in range(5, half) for o in around(s)] + [0])
    halos = {}

    def send_piece(i):
        packed = pack(near_x if i else x, pieces[i], i > 0)
        got = passed_along(packed, "tm", 1, False)
        halos.update({o: (got, place) for place, o in enumerate(pieces[i])})

    def own(offsets, split_rows, dtype):
        parts = []
        for j, o in enumerate(offsets):
            spots = [(j, q) for q in range(rows)]
            if split_rows:
                spots = [(0, q) if q < split else (1, q - split) for q in range(rows)]
            parts.append((o, halos[o][1], spots))
        return beams_of(
            parts, split if split_rows else rows, dtype, tap_sets, near_x, near_w, banks, halos[o][0]
        )

    send_piece(0)
    *banks, near_x, near_w = bank(tap_table, delays, x, w)
    right, left = own([half], True, jnp.bfloat16)
    send_piece(1)
    send_piece(2)
    for s in range(1, half + 1):
        right = passed_along(right, "station", 1, True)
        left = passed_along(left, "station", -1, True)
        if s == half:
            return finish(right, left, own([0], False, jnp.float32)[0])
        own_right, own_left = own(around(s), False, jnp.float32)
        if s == 1:
            right, left = join(right, left, own_right, own_left)
        else:
            right = (right.astype(jnp.float32) + own_right).astype(jnp.bfloat16)
            left = (left.astype(jnp.float32) + own_left).astype(jnp.bfloat16)


def solution(mesh):
    return jax.shard_map(
        ring,
        mesh=mesh,
        in_specs=(
            P(("group", "station"), "chan", None, None, "tm"),
            P(("group", "station")),
            P(("group", "station"), "chan"),
            P(),
            P(("group", "station"), "chan", None, None, None),
        ),
        out_specs=P(("group", "chan", "station"), None, None, "tm"),
        check_vma=False,
    )
```

```python
import functools

import jax
import jax.numpy as jnp
from jax import lax
from jax.experimental import pallas as pl
from jax.experimental.pallas import tpu as pltpu
from jax.sharding import PartitionSpec as P


TAPS = 16
HALO = 32


ANY = pl.BlockSpec(memory_space=pl.ANY)
VMEM = pl.BlockSpec(memory_space=pltpu.VMEM)
SMEM = pl.BlockSpec(memory_space=pltpu.SMEM)
PARAMS = pltpu.CompilerParams(vmem_limit_bytes=6 * 1024 * 1024)


def near(value, space=pltpu.VMEM):
    return pltpu.with_memory_space_constraint(value, space)


def from_earlier(value):
    return lax.ppermute(value, "tm", [(i, i + 1) for i in range(lax.axis_size("tm") - 1)])


def onward(value):
    count, cores = lax.axis_size("station"), lax.axis_size("chan")
    pairs = []
    for station in range(count):
        for core in range(cores):
            step = 1 if core % 2 == 0 else -1
            pairs.append((station * cores + core, (station + step) % count * cores + core))
    return lax.ppermute(value, ("station", "chan"), pairs)


def across_cores(value):
    cores = lax.axis_size("chan")
    return lax.ppermute(value, "chan", [(i, (i + 1) % cores) for i in range(cores)])


def chunk_index(offset, count):
    up = lax.rem(lax.axis_index("chan"), 2) == 0
    signed = jnp.where(up, offset % count, -offset % count)
    return lax.rem(lax.axis_index("station") + signed, count)


def side_by_side(channels):
    return jnp.concatenate([one[:, one.shape[-1] - HALO :] for one in channels], axis=-1)


def pack_near_kernel(offsets, count, x_ref, packed_ref):
    for i, offset in enumerate(offsets):
        chunk = chunk_index(offset, count)
        packed_ref[i] = side_by_side([x_ref[chunk, q] for q in range(x_ref.shape[1])])


def pack_kernel(offsets, count, x_ref, packed_ref, buf, sem):
    copies = [
        pltpu.make_async_copy(x_ref.at[chunk_index(offset, count)], buf.at[i], sem.at[i])
        for i, offset in enumerate(offsets)
    ]
    for copy in copies:
        copy.start()
    for i, copy in enumerate(copies):
        copy.wait()
        packed_ref[i] = side_by_side([buf[i, q] for q in range(buf.shape[1])])


def pack(x, offsets, direct):
    count, rows, height, length = x.shape
    shape = pltpu.VMEM((len(offsets), height, rows * HALO), x.dtype)
    if direct:
        return pl.pallas_call(
            functools.partial(pack_near_kernel, offsets, count),
            out_shape=shape,
            in_specs=[VMEM],
            out_specs=VMEM,
            compiler_params=PARAMS,
            name="pack",
        )(near(x))
    return pl.pallas_call(
        functools.partial(pack_kernel, offsets, count),
        out_shape=shape,
        in_specs=[ANY],
        out_specs=VMEM,
        scratch_shapes=[
            pltpu.VMEM((len(offsets), rows, height, length), x.dtype),
            pltpu.SemaphoreType.DMA((len(offsets),)),
        ],
        compiler_params=PARAMS,
        name="pack",
    )(near(x, pltpu.HBM))


def bank_kernel(
    offsets, count, delay_ref, table_ref, x_ref, w_ref,
    main_ref, edge_ref, near_x_ref, near_w_ref, packed_ref, sem,
):
    sets, length, _ = main_ref.shape
    copies = [
        pltpu.make_async_copy(x_ref, near_x_ref, sem.at[0]),
        pltpu.make_async_copy(w_ref, near_w_ref, sem.at[1]),
    ]
    for copy in copies:
        copy.start()
    tap = lax.broadcasted_iota(jnp.int32, (TAPS, length), 0)
    lane = lax.broadcasted_iota(jnp.int32, (TAPS, length), 1)
    back = delay_ref[0] + lane + tap
    hit = ((back == 0) | (back == length)).astype(jnp.bfloat16)
    first_rows = jnp.dot(table_ref[...], hit, preferred_element_type=jnp.float32)
    row = lax.broadcasted_iota(jnp.int32, (length, length), 0)
    own = lax.broadcasted_iota(jnp.int32, (length, length), 1) <= row
    lanes = lax.broadcasted_iota(jnp.int32, (HALO, length), 1)
    for m in range(sets):
        band = jnp.broadcast_to(first_rows[m : m + 1], (length, length))
        band = pltpu.roll(band, 0, 1, stride=1, stride_axis=0)
        main_ref[m] = jnp.where(own, band, 0.0).astype(main_ref.dtype)
        edge = jnp.where(lanes >= length - HALO, band[:HALO], 0.0)
        spread = edge
        for q in range(1, length // HALO):
            spread = spread + pltpu.roll(edge, q * HALO, 1)
        edge_ref[m] = spread.astype(edge_ref.dtype)
    for copy in copies:
        copy.wait()
    pack_near_kernel(offsets, count, near_x_ref, packed_ref)


def bank(table, delays, x, w, offsets):
    _, rows, height, length = x.shape
    sets = table.shape[0]
    return pl.pallas_call(
        functools.partial(bank_kernel, offsets, x.shape[0]),
        out_shape=(
            pltpu.VMEM((sets, length, length), jnp.bfloat16),
            pltpu.VMEM((sets, HALO, length), jnp.bfloat16),
            pltpu.VMEM(x.shape, x.dtype),
            pltpu.VMEM(w.shape, w.dtype),
            pltpu.VMEM((len(offsets), height, rows * HALO), x.dtype),
        ),
        in_specs=[SMEM, VMEM, ANY, ANY],
        out_specs=(VMEM,) * 5,
        scratch_shapes=[pltpu.SemaphoreType.DMA((2,))],
        compiler_params=PARAMS,
        name="bank",
    )(near(delays, pltpu.SMEM), table, near(x, pltpu.HBM), near(w, pltpu.HBM))


def settle_kernel(offsets, count, value_ref, *refs):
    out_ref, sem = refs[-2:]
    if offsets:
        copies = [
            pltpu.make_async_copy(value_ref.at[chunk_index(o, count)], out_ref.at[i], sem.at[i])
            for i, o in enumerate(offsets)
        ]
    else:
        copies = [pltpu.make_async_copy(value_ref, out_ref, sem.at[0])]
    for copy in copies:
        copy.start()
    for copy in copies:
        copy.wait()


def settle(value, offsets=(), after=()):
    shape = (len(offsets),) + value.shape[1:] if offsets else value.shape
    return pl.pallas_call(
        functools.partial(settle_kernel, offsets, value.shape[0]),
        out_shape=pltpu.VMEM(shape, value.dtype),
        in_specs=[ANY] + [VMEM] * len(after),
        out_specs=VMEM,
        scratch_shapes=[pltpu.SemaphoreType.DMA((max(1, len(offsets)),))],
        compiler_params=PARAMS,
        name="settle",
    )(value, *[near(one) for one in after])


FILTER, STEER, BOTH = range(3)


def work_kernel(jobs, count, rows, names, *refs):
    held = dict(zip(names, refs))
    outs = refs[len(names) :]
    nt = (((1,), (1,)), ((), ()))
    filters = 0
    for i, (what, offset, place) in enumerate(jobs):
        out = outs[-1].at[filters] if what == FILTER else outs[i]
        filters += what == FILTER
        chunk = chunk_index(offset, count)
        if what != STEER:
            x_ref = held["x"].at[chunk]
            length = x_ref.shape[-1]
            lane_block = lax.broadcasted_iota(jnp.int32, (HALO, length), 1) // HALO
            chosen = [held["sets"][0, chunk * rows + q] for q in range(rows)]
            edge = jnp.concatenate(
                [
                    jnp.where(lane_block == q, held["edge"][m], jnp.zeros((), jnp.bfloat16))
                    for q, m in enumerate(chosen)
                ],
                axis=0,
            )
            early = lax.dot_general(
                edge, held["halo"][place], nt, preferred_element_type=jnp.float32
            )
        w_ref = None
        if what == BOTH:
            w_ref = held["w"].at[chunk]
        elif what == STEER:
            w_ref = held["other_w"].at[held["other_w"].shape[0] - offset]
        for q in range(rows):
            if what == STEER:
                delayed = held["given"][place, q, :, : 2 * w_ref.shape[-2]]
            else:
                late = lax.dot_general(
                    held["main"][chosen[q]], x_ref[q], nt, preferred_element_type=jnp.float32
                )
                delayed = jnp.concatenate(
                    [late[:HALO] + early[q * HALO : (q + 1) * HALO], late[HALO:]], axis=0
                ).astype(jnp.bfloat16)
            if what == FILTER:
                spare = jnp.zeros((delayed.shape[0], out.shape[-1] - delayed.shape[1]), out.dtype)
                out[q] = jnp.concatenate([delayed, spare], axis=-1)
                continue
            real_w = w_ref[q, 0]
            imag_w = w_ref[q, 1]
            steer = jnp.concatenate(
                [
                    jnp.concatenate([real_w, imag_w], axis=-1),
                    jnp.concatenate([-imag_w, real_w], axis=-1),
                ],
                axis=0,
            )
            out[q] = jnp.dot(delayed, steer, preferred_element_type=jnp.float32).astype(out.dtype)


def work(jobs, dtypes, rows, count, length, height, width, **arrays):
    names = tuple(arrays)
    shapes = [pltpu.VMEM((rows, length, width), dtype) for dtype in dtypes]
    filters = sum(what == FILTER for what, _, _ in jobs)
    if filters:
        lanes = (height + 127) // 128 * 128
        shapes.append(pltpu.VMEM((filters, rows, length, lanes), jnp.bfloat16))
    flops = 0
    for what, _, _ in jobs:
        flops += 2 * rows * length * height * (
            (0 if what == STEER else length) + (0 if what == FILTER else width)
        )
    return pl.pallas_call(
        functools.partial(work_kernel, jobs, count, rows, names),
        out_shape=tuple(shapes),
        in_specs=[SMEM if name == "sets" else VMEM for name in names],
        out_specs=(VMEM,) * len(shapes),
        cost_estimate=pl.CostEstimate(flops=flops, bytes_accessed=flops // 256, transcendentals=0),
        compiler_params=PARAMS,
        name="work",
    )(*[near(value, pltpu.SMEM if name == "sets" else pltpu.VMEM) for name, value in arrays.items()])


def finish_kernel(right_ref, left_ref, own_ref, out_ref):
    rows, _, width = own_ref.shape
    half = width // 2
    for q in range(rows):
        total = (
            right_ref[q].astype(jnp.float32) + left_ref[q].astype(jnp.float32) + own_ref[q]
        )
        for part in range(2):
            out_ref[q, part] = total[:, part * half : (part + 1) * half].T.astype(out_ref.dtype)


def finish(right, left, own):
    rows, length, width = own.shape
    return pl.pallas_call(
        finish_kernel,
        out_shape=jax.ShapeDtypeStruct((rows, 2, width // 2, length), jnp.bfloat16),
        in_specs=[VMEM] * 3,
        out_specs=VMEM,
        compiler_params=PARAMS,
        name="finish",
    )(near(right), near(left), near(own))


def ring(voltages, delays, tap_sets, tap_table, weights):
    _, channels, pair, antennas, length = voltages.shape
    beam_count = weights.shape[-1]
    count = lax.axis_size("station")
    rows = channels // count
    half = count // 2
    height = pair * antennas
    x = voltages.reshape(count, rows, height, length)
    w = weights.reshape(count, rows, pair, antennas, beam_count)
    sizes = (rows, count, length, height, 2 * beam_count)
    wide, thin = jnp.float32, jnp.bfloat16

    pieces = [[half, half - 1, 1 - half]]
    pieces.append([o for s in (2, 3) for o in (half - s, s - half)])
    pieces.append([o for s in range(4, half) for o in (half - s, s - half)] + [0])
    halos = {}

    def use_piece(i, got, after=()):
        if after:
            got = settle(got, (), after)
        halos.update({o: (got, place) for place, o in enumerate(pieces[i])})

    packed = pack(x, pieces[0], False)
    use_piece(0, from_earlier(packed))
    main, edge, near_x, near_w, packed = bank(tap_table, delays, x, w, pieces[1])
    other_w = across_cores(w)
    second = packed
    common = {"sets": tap_sets, "main": main, "edge": edge, "x": near_x, "w": near_w}

    def filtered(offsets):
        jobs = tuple((FILTER, o, halos[o][1]) for o in offsets)
        return work(jobs, [], *sizes, **common, halo=halos[offsets[0]][0])[0]

    halo, place = halos[half]
    a, handed = work(
        ((BOTH, half, place), (FILTER, 1 - half, halos[1 - half][1])), [thin],
        *sizes, **common, halo=halo,
    )
    a_got = onward(a)
    given = {1: (across_cores(handed), 0)}
    other_w = settle(other_w, tuple(half - s for s in range(1, half)))
    halo, place = halos[half - 1]
    (own,) = work(((BOTH, half - 1, place),), [wide], *sizes, **common, halo=halo)
    second = from_earlier(second)
    packed = pack(near_x, pieces[2], True)
    (b,) = work(
        ((STEER, half - 1, 0),), [thin], *sizes, given=given[1][0], other_w=other_w
    )

    def send_filtered(first, last):
        over = filtered([s - half for s in range(first, last)])
        got = across_cores(over)
        got = settle(got)
        given.update({s: (got, s - first) for s in range(first, last)})

    for s in range(1, half):
        b_got = onward(b)
        a = (a_got.astype(wide) + own).astype(thin)
        a_got = onward(a)
        if s == 1:
            use_piece(1, second, (b,))
            send_filtered(2, 4)
            third = from_earlier(packed)
        elif s == 3:
            use_piece(2, third, (a, b))
            send_filtered(4, half)
        halo, place = halos[half - s - 1]
        if s == half - 1:
            (own,) = work(((BOTH, 0, place),), [wide], *sizes, **common, halo=halo)
            break
        job = (BOTH, half - s - 1, place)
        if s != 3:
            own, other = work(
                (job, (STEER, half - s - 1, given[s + 1][1])), [wide, wide], *sizes, **common,
                halo=halo, given=given[s + 1][0], other_w=other_w,
            )
        else:
            (own,) = work((job,), [wide], *sizes, **common, halo=halo)
            (other,) = work(
                ((STEER, half - s - 1, given[s + 1][1]),), [wide], *sizes,
                given=given[s + 1][0], other_w=other_w,
            )
        b = (b_got.astype(wide) + other).astype(thin)
    back = across_cores(b_got)
    return finish(a_got, back, own)


def solution(mesh):
    return jax.shard_map(
        ring,
        mesh=mesh,
        in_specs=(
            P(("group", "station"), "chan", None, None, "tm"),
            P(("group", "station")),
            P(("group", "station"), "chan"),
            P(),
            P(("group", "station"), "chan", None, None, None),
        ),
        out_specs=P(("group", "chan", "station"), None, None, "tm"),
        check_vma=False,
    )
```

```python
import functools

import jax
import jax.numpy as jnp
from jax import lax
from jax.experimental import pallas as pl
from jax.experimental.pallas import tpu as pltpu
from jax.sharding import PartitionSpec as P


TAPS = 16
HALO = 32


ANY = pl.BlockSpec(memory_space=pl.ANY)
VMEM = pl.BlockSpec(memory_space=pltpu.VMEM)
SMEM = pl.BlockSpec(memory_space=pltpu.SMEM)
PARAMS = pltpu.CompilerParams(vmem_limit_bytes=6 * 1024 * 1024)


def near(value, space=pltpu.VMEM):
    return pltpu.with_memory_space_constraint(value, space)


def from_earlier(value):
    return lax.ppermute(value, "tm", [(i, i + 1) for i in range(lax.axis_size("tm") - 1)])


def onward(value):
    count, cores = lax.axis_size("station"), lax.axis_size("chan")
    pairs = []
    for station in range(count):
        for core in range(cores):
            step = 1 if core % 2 == 0 else -1
            pairs.append((station * cores + core, (station + step) % count * cores + core))
    return lax.ppermute(value, ("station", "chan"), pairs)


def across_cores(value):
    cores = lax.axis_size("chan")
    return lax.ppermute(value, "chan", [(i, (i + 1) % cores) for i in range(cores)])


def chunk_index(offset, count):
    up = lax.rem(lax.axis_index("chan"), 2) == 0
    signed = jnp.where(up, offset % count, -offset % count)
    return lax.rem(lax.axis_index("station") + signed, count)


def side_by_side(channels):
    return jnp.concatenate([one[:, one.shape[-1] - HALO :] for one in channels], axis=-1)


def pack_near_kernel(offsets, count, x_ref, packed_ref):
    for i, offset in enumerate(offsets):
        chunk = chunk_index(offset, count)
        packed_ref[i] = side_by_side([x_ref[chunk, q] for q in range(x_ref.shape[1])])


def pack_kernel(offsets, count, x_ref, packed_ref, buf, sem):
    copies = [
        pltpu.make_async_copy(x_ref.at[chunk_index(offset, count)], buf.at[i], sem.at[i])
        for i, offset in enumerate(offsets)
    ]
    for copy in copies:
        copy.start()
    for i, copy in enumerate(copies):
        copy.wait()
        packed_ref[i] = side_by_side([buf[i, q] for q in range(buf.shape[1])])


def pack(x, offsets, direct):
    count, rows, height, length = x.shape
    shape = pltpu.VMEM((len(offsets), height, rows * HALO), x.dtype)
    if direct:
        return pl.pallas_call(
            functools.partial(pack_near_kernel, offsets, count),
            out_shape=shape,
            in_specs=[VMEM],
            out_specs=VMEM,
            compiler_params=PARAMS,
            name="pack",
        )(near(x))
    return pl.pallas_call(
        functools.partial(pack_kernel, offsets, count),
        out_shape=shape,
        in_specs=[ANY],
        out_specs=VMEM,
        scratch_shapes=[
            pltpu.VMEM((len(offsets), rows, height, length), x.dtype),
            pltpu.SemaphoreType.DMA((len(offsets),)),
        ],
        compiler_params=PARAMS,
        name="pack",
    )(near(x, pltpu.HBM))


def bank_kernel(
    offsets, count, delay_ref, table_ref, x_ref,
    main_ref, edge_ref, near_x_ref, packed_ref, sem,
):
    sets, length, _ = main_ref.shape
    copy = pltpu.make_async_copy(x_ref, near_x_ref, sem)
    copy.start()
    tap = lax.broadcasted_iota(jnp.int32, (TAPS, length), 0)
    lane = lax.broadcasted_iota(jnp.int32, (TAPS, length), 1)
    back = delay_ref[0] + lane + tap
    hit = ((back == 0) | (back == length)).astype(jnp.bfloat16)
    first_rows = jnp.dot(table_ref[...], hit, preferred_element_type=jnp.float32)
    row = lax.broadcasted_iota(jnp.int32, (length, length), 0)
    own = lax.broadcasted_iota(jnp.int32, (length, length), 1) <= row
    lanes = lax.broadcasted_iota(jnp.int32, (HALO, length), 1)
    for m in range(sets):
        band = jnp.broadcast_to(first_rows[m : m + 1], (length, length))
        band = pltpu.roll(band, 0, 1, stride=1, stride_axis=0)
        main_ref[m] = jnp.where(own, band, 0.0).astype(main_ref.dtype)
        edge = jnp.where(lanes >= length - HALO, band[:HALO], 0.0)
        spread = edge
        for q in range(1, length // HALO):
            spread = spread + pltpu.roll(edge, q * HALO, 1)
        edge_ref[m] = spread.astype(edge_ref.dtype)
    copy.wait()
    pack_near_kernel(offsets, count, near_x_ref, packed_ref)


def bank(table, delays, x, offsets):
    _, rows, height, length = x.shape
    sets = table.shape[0]
    return pl.pallas_call(
        functools.partial(bank_kernel, offsets, x.shape[0]),
        out_shape=(
            pltpu.VMEM((sets, length, length), jnp.bfloat16),
            pltpu.VMEM((sets, HALO, length), jnp.bfloat16),
            pltpu.VMEM(x.shape, x.dtype),
            pltpu.VMEM((len(offsets), height, rows * HALO), x.dtype),
        ),
        in_specs=[SMEM, VMEM, ANY],
        out_specs=(VMEM,) * 4,
        scratch_shapes=[pltpu.SemaphoreType.DMA],
        compiler_params=PARAMS,
        name="bank",
    )(near(delays, pltpu.SMEM), table, near(x, pltpu.HBM))


def settle_kernel(value_ref, *refs):
    out_ref, sem = refs[-2:]
    copy = pltpu.make_async_copy(value_ref, out_ref, sem)
    copy.start()
    copy.wait()


def settle(value, after=()):
    return pl.pallas_call(
        settle_kernel,
        out_shape=pltpu.VMEM(value.shape, value.dtype),
        in_specs=[ANY] + [VMEM] * len(after),
        out_specs=VMEM,
        scratch_shapes=[pltpu.SemaphoreType.DMA],
        compiler_params=PARAMS,
        name="settle",
    )(value, *[near(one) for one in after])


FILTER, STEER, BOTH = range(3)


def work_kernel(jobs, count, rows, names, fetch, *refs):
    held = dict(zip(names, refs))
    outs = refs[len(names) :]
    copies = []
    if fetch:
        *outs, near_ref, sem = outs
        copies = [
            pltpu.make_async_copy(held["raw"].at[chunk_index(o, count)], near_ref.at[i], sem.at[i])
            for i, o in enumerate(fetch)
        ]
        for copy in copies:
            copy.start()
    nt = (((1,), (1,)), ((), ()))
    filters = 0
    for i, (what, offset, place) in enumerate(jobs):
        out = outs[-1].at[filters] if what == FILTER else outs[i]
        filters += what == FILTER
        chunk = chunk_index(offset, count)
        if what != STEER:
            x_ref = held["x"].at[chunk]
            length = x_ref.shape[-1]
            lane_block = lax.broadcasted_iota(jnp.int32, (HALO, length), 1) // HALO
            chosen = [held["sets"][0, chunk * rows + q] for q in range(rows)]
            edge = jnp.concatenate(
                [
                    jnp.where(lane_block == q, held["edge"][m], jnp.zeros((), jnp.bfloat16))
                    for q, m in enumerate(chosen)
                ],
                axis=0,
            )
            early = lax.dot_general(
                edge, held["halo"][place], nt, preferred_element_type=jnp.float32
            )
        w_ref = None
        if what == BOTH:
            w_ref = held["w"].at[chunk]
        elif what == STEER:
            w_ref = held["other_w"].at[held["other_w"].shape[0] - offset]
        for q in range(rows):
            if what == STEER:
                delayed = held["given"][place, q, :, : 2 * w_ref.shape[-2]]
            else:
                late = lax.dot_general(
                    held["main"][chosen[q]], x_ref[q], nt, preferred_element_type=jnp.float32
                )
                delayed = jnp.concatenate(
                    [late[:HALO] + early[q * HALO : (q + 1) * HALO], late[HALO:]], axis=0
                ).astype(jnp.bfloat16)
            if what == FILTER:
                spare = jnp.zeros((delayed.shape[0], out.shape[-1] - delayed.shape[1]), out.dtype)
                out[q] = jnp.concatenate([delayed, spare], axis=-1)
                continue
            real_w = w_ref[q, 0]
            imag_w = w_ref[q, 1]
            steer = jnp.concatenate(
                [
                    jnp.concatenate([real_w, imag_w], axis=-1),
                    jnp.concatenate([-imag_w, real_w], axis=-1),
                ],
                axis=0,
            )
            out[q] = jnp.dot(delayed, steer, preferred_element_type=jnp.float32).astype(out.dtype)
    for copy in copies:
        copy.wait()


def work(jobs, dtypes, rows, count, length, height, width, fetch=(), **arrays):
    names = tuple(arrays)
    shapes = [pltpu.VMEM((rows, length, width), dtype) for dtype in dtypes]
    filters = sum(what == FILTER for what, _, _ in jobs)
    if filters:
        lanes = (height + 127) // 128 * 128
        shapes.append(pltpu.VMEM((filters, rows, length, lanes), jnp.bfloat16))
    if fetch:
        shapes.append(pltpu.VMEM((len(fetch),) + arrays["raw"].shape[1:], arrays["raw"].dtype))
    flops = 0
    for what, _, _ in jobs:
        flops += 2 * rows * length * height * (
            (0 if what == STEER else length) + (0 if what == FILTER else width)
        )
    return pl.pallas_call(
        functools.partial(work_kernel, jobs, count, rows, names, fetch),
        out_shape=tuple(shapes),
        in_specs=[{"sets": SMEM, "raw": ANY}.get(name, VMEM) for name in names],
        out_specs=(VMEM,) * len(shapes),
        scratch_shapes=[pltpu.SemaphoreType.DMA((len(fetch),))] if fetch else [],
        cost_estimate=pl.CostEstimate(flops=flops, bytes_accessed=flops // 256, transcendentals=0),
        compiler_params=PARAMS,
        name="work",
    )(
        *[
            value if name == "raw" else near(value, pltpu.SMEM if name == "sets" else pltpu.VMEM)
            for name, value in arrays.items()
        ]
    )


def finish_kernel(right_ref, left_ref, own_ref, out_ref):
    rows, _, width = own_ref.shape
    half = width // 2
    for q in range(rows):
        total = (
            right_ref[q].astype(jnp.float32) + left_ref[q].astype(jnp.float32) + own_ref[q]
        )
        for part in range(2):
            out_ref[q, part] = total[:, part * half : (part + 1) * half].T.astype(out_ref.dtype)


def finish(right, left, own):
    rows, length, width = own.shape
    return pl.pallas_call(
        finish_kernel,
        out_shape=jax.ShapeDtypeStruct((rows, 2, width // 2, length), jnp.bfloat16),
        in_specs=[VMEM] * 3,
        out_specs=VMEM,
        compiler_params=PARAMS,
        name="finish",
    )(near(right), near(left), near(own))


def ring(voltages, delays, tap_sets, tap_table, weights):
    _, channels, pair, antennas, length = voltages.shape
    beam_count = weights.shape[-1]
    count = lax.axis_size("station")
    rows = channels // count
    half = count // 2
    height = pair * antennas
    x = voltages.reshape(count, rows, height, length)
    w = weights.reshape(count, rows, pair, antennas, beam_count)
    sizes = (rows, count, length, height, 2 * beam_count)
    wide, thin = jnp.float32, jnp.bfloat16

    pieces = [[half, half - 1, 1 - half]]
    pieces.append([o for s in (2, 3) for o in (half - s, s - half)])
    pieces.append([o for s in range(4, half) for o in (half - s, s - half)] + [0])
    halos = {}

    def use_piece(i, got, after=()):
        if after:
            got = settle(got, after)
        halos.update({o: (got, place) for place, o in enumerate(pieces[i])})

    packed = pack(x, pieces[0], False)
    use_piece(0, from_earlier(packed))
    main, edge, near_x, packed = bank(tap_table, delays, x, pieces[1])
    other_w = across_cores(w)
    second = packed
    common = {"sets": tap_sets, "main": main, "edge": edge, "x": near_x, "w": w}

    def filtered(offsets):
        jobs = tuple((FILTER, o, halos[o][1]) for o in offsets)
        return work(jobs, [], *sizes, **common, halo=halos[offsets[0]][0])[0]

    halo, place = halos[half]
    a, handed = work(
        ((BOTH, half, place), (FILTER, 1 - half, halos[1 - half][1])), [thin],
        *sizes, **common, halo=halo,
    )
    a_got = onward(a)
    given = {1: (across_cores(handed), 0)}
    halo, place = halos[half - 1]
    own, other_w = work(
        ((BOTH, half - 1, place),), [wide], *sizes, **common, halo=halo,
        fetch=tuple(half - s for s in range(1, half)), raw=other_w,
    )
    second = from_earlier(second)
    packed = pack(near_x, pieces[2], True)
    (b,) = work(
        ((STEER, half - 1, 0),), [thin], *sizes, given=given[1][0], other_w=other_w
    )

    def send_filtered(first, last):
        over = filtered([s - half for s in range(first, last)])
        got = across_cores(over)
        got = settle(got)
        given.update({s: (got, s - first) for s in range(first, last)})

    for s in range(1, half):
        b_got = onward(b)
        a = (a_got.astype(wide) + own).astype(thin)
        a_got = onward(a)
        if s == 1:
            use_piece(1, second, (a, b))
            send_filtered(2, 4)
            third = from_earlier(packed)
        elif s == 3:
            use_piece(2, third, (a, b))
            send_filtered(4, half)
        halo, place = halos[half - s - 1]
        if s == half - 1:
            (own,) = work(((BOTH, 0, place),), [wide], *sizes, **common, halo=halo)
            break
        job = (BOTH, half - s - 1, place)
        if s != 3:
            own, other = work(
                (job, (STEER, half - s - 1, given[s + 1][1])), [wide, wide], *sizes, **common,
                halo=halo, given=given[s + 1][0], other_w=other_w,
            )
        else:
            (own,) = work((job,), [wide], *sizes, **common, halo=halo)
            (other,) = work(
                ((STEER, half - s - 1, given[s + 1][1]),), [wide], *sizes,
                given=given[s + 1][0], other_w=other_w,
            )
        b = (b_got.astype(wide) + other).astype(thin)
    back = across_cores(b_got)
    return finish(a_got, back, own)


def solution(mesh):
    return jax.shard_map(
        ring,
        mesh=mesh,
        in_specs=(
            P(("group", "station"), "chan", None, None, "tm"),
            P(("group", "station")),
            P(("group", "station"), "chan"),
            P(),
            P(("group", "station"), "chan", None, None, None),
        ),
        out_specs=P(("group", "chan", "station"), None, None, "tm"),
        check_vma=False,
    )
```

```python
import functools

import jax
import jax.numpy as jnp
from jax import lax
from jax.experimental import pallas as pl
from jax.experimental.pallas import tpu as pltpu
from jax.sharding import PartitionSpec as P


TAPS = 16
HALO = 32


ANY = pl.BlockSpec(memory_space=pl.ANY)
VMEM = pl.BlockSpec(memory_space=pltpu.VMEM)
SMEM = pl.BlockSpec(memory_space=pltpu.SMEM)
PARAMS = pltpu.CompilerParams(vmem_limit_bytes=6 * 1024 * 1024)


def near(value, space=pltpu.VMEM):
    return pltpu.with_memory_space_constraint(value, space)


def from_earlier(value):
    return lax.ppermute(value, "tm", [(i, i + 1) for i in range(lax.axis_size("tm") - 1)])


def onward(value):
    count, cores = lax.axis_size("station"), lax.axis_size("chan")
    pairs = []
    for station in range(count):
        for core in range(cores):
            step = 1 if core % 2 == 0 else -1
            pairs.append((station * cores + core, (station + step) % count * cores + core))
    return lax.ppermute(value, ("station", "chan"), pairs)


def across_cores(value):
    cores = lax.axis_size("chan")
    return lax.ppermute(value, "chan", [(i, (i + 1) % cores) for i in range(cores)])


def chunk_index(offset, count):
    up = lax.rem(lax.axis_index("chan"), 2) == 0
    signed = jnp.where(up, offset % count, -offset % count)
    return lax.rem(lax.axis_index("station") + signed, count)


def side_by_side(channels):
    return jnp.concatenate([one[:, one.shape[-1] - HALO :] for one in channels], axis=-1)


def pack_near_kernel(offsets, count, x_ref, packed_ref):
    for i, offset in enumerate(offsets):
        chunk = chunk_index(offset, count)
        packed_ref[i] = side_by_side([x_ref[chunk, q] for q in range(x_ref.shape[1])])


def pack_kernel(offsets, count, x_ref, packed_ref, buf, sem):
    copies = [
        pltpu.make_async_copy(x_ref.at[chunk_index(offset, count)], buf.at[i], sem.at[i])
        for i, offset in enumerate(offsets)
    ]
    for copy in copies:
        copy.start()
    for i, copy in enumerate(copies):
        copy.wait()
        packed_ref[i] = side_by_side([buf[i, q] for q in range(buf.shape[1])])


def pack(x, offsets, direct):
    count, rows, height, length = x.shape
    shape = pltpu.VMEM((len(offsets), height, rows * HALO), x.dtype)
    if direct:
        return pl.pallas_call(
            functools.partial(pack_near_kernel, offsets, count),
            out_shape=shape,
            in_specs=[VMEM],
            out_specs=VMEM,
            compiler_params=PARAMS,
            name="pack",
        )(near(x))
    return pl.pallas_call(
        functools.partial(pack_kernel, offsets, count),
        out_shape=shape,
        in_specs=[ANY],
        out_specs=VMEM,
        scratch_shapes=[
            pltpu.VMEM((len(offsets), rows, height, length), x.dtype),
            pltpu.SemaphoreType.DMA((len(offsets),)),
        ],
        compiler_params=PARAMS,
        name="pack",
    )(near(x, pltpu.HBM))


def bank_kernel(
    offsets, count, delay_ref, table_ref, x_ref,
    main_ref, edge_ref, near_x_ref, packed_ref, sem,
):
    sets, length, _ = main_ref.shape
    copy = pltpu.make_async_copy(x_ref, near_x_ref, sem)
    copy.start()
    tap = lax.broadcasted_iota(jnp.int32, (TAPS, length), 0)
    lane = lax.broadcasted_iota(jnp.int32, (TAPS, length), 1)
    back = delay_ref[0] + lane + tap
    hit = ((back == 0) | (back == length)).astype(jnp.bfloat16)
    first_rows = jnp.dot(table_ref[...], hit, preferred_element_type=jnp.float32)
    row = lax.broadcasted_iota(jnp.int32, (length, length), 0)
    own = lax.broadcasted_iota(jnp.int32, (length, length), 1) <= row
    lanes = lax.broadcasted_iota(jnp.int32, (HALO, length), 1)
    for m in range(sets):
        band = jnp.broadcast_to(first_rows[m : m + 1], (length, length))
        band = pltpu.roll(band, 0, 1, stride=1, stride_axis=0)
        main_ref[m] = jnp.where(own, band, 0.0).astype(main_ref.dtype)
        edge = jnp.where(lanes >= length - HALO, band[:HALO], 0.0)
        spread = edge
        for q in range(1, length // HALO):
            spread = spread + pltpu.roll(edge, q * HALO, 1)
        edge_ref[m] = spread.astype(edge_ref.dtype)
    copy.wait()
    pack_near_kernel(offsets, count, near_x_ref, packed_ref)


def bank(table, delays, x, offsets):
    _, rows, height, length = x.shape
    sets = table.shape[0]
    return pl.pallas_call(
        functools.partial(bank_kernel, offsets, x.shape[0]),
        out_shape=(
            pltpu.VMEM((sets, length, length), jnp.bfloat16),
            pltpu.VMEM((sets, HALO, length), jnp.bfloat16),
            pltpu.VMEM(x.shape, x.dtype),
            pltpu.VMEM((len(offsets), height, rows * HALO), x.dtype),
        ),
        in_specs=[SMEM, VMEM, ANY],
        out_specs=(VMEM,) * 4,
        scratch_shapes=[pltpu.SemaphoreType.DMA],
        compiler_params=PARAMS,
        name="bank",
    )(near(delays, pltpu.SMEM), table, near(x, pltpu.HBM))


def settle_kernel(value_ref, *refs):
    out_ref, sem = refs[-2:]
    copy = pltpu.make_async_copy(value_ref, out_ref, sem)
    copy.start()
    copy.wait()


def settle(value, after=()):
    return pl.pallas_call(
        settle_kernel,
        out_shape=pltpu.VMEM(value.shape, value.dtype),
        in_specs=[ANY] + [VMEM] * len(after),
        out_specs=VMEM,
        scratch_shapes=[pltpu.SemaphoreType.DMA],
        compiler_params=PARAMS,
        name="settle",
    )(value, *[near(one) for one in after])


FILTER, STEER, BOTH = range(3)


def work_kernel(jobs, count, rows, names, *refs):
    held = dict(zip(names, refs))
    outs = refs[len(names) :]
    nt = (((1,), (1,)), ((), ()))
    filters = 0
    for i, (what, offset, place) in enumerate(jobs):
        out = outs[-1].at[filters] if what == FILTER else outs[i]
        filters += what == FILTER
        chunk = chunk_index(offset, count)
        if what != STEER:
            x_ref = held["x"].at[chunk]
            length = x_ref.shape[-1]
            lane_block = lax.broadcasted_iota(jnp.int32, (HALO, length), 1) // HALO
            chosen = [held["sets"][0, chunk * rows + q] for q in range(rows)]
            edge = jnp.concatenate(
                [
                    jnp.where(lane_block == q, held["edge"][m], jnp.zeros((), jnp.bfloat16))
                    for q, m in enumerate(chosen)
                ],
                axis=0,
            )
            early = lax.dot_general(
                edge, held["halo"][place], nt, preferred_element_type=jnp.float32
            )
        w_ref = None
        if what == BOTH:
            w_ref = held["w"].at[chunk]
        elif what == STEER:
            w_ref = held["other_w"].at[chunk]
        for q in range(rows):
            if what == STEER:
                delayed = held["given"][place, q, :, : 2 * w_ref.shape[-2]]
            else:
                late = lax.dot_general(
                    held["main"][chosen[q]], x_ref[q], nt, preferred_element_type=jnp.float32
                )
                delayed = jnp.concatenate(
                    [late[:HALO] + early[q * HALO : (q + 1) * HALO], late[HALO:]], axis=0
                ).astype(jnp.bfloat16)
            if what == FILTER:
                spare = jnp.zeros((delayed.shape[0], out.shape[-1] - delayed.shape[1]), out.dtype)
                out[q] = jnp.concatenate([delayed, spare], axis=-1)
                continue
            real_w = w_ref[q, 0]
            imag_w = w_ref[q, 1]
            steer = jnp.concatenate(
                [
                    jnp.concatenate([real_w, imag_w], axis=-1),
                    jnp.concatenate([-imag_w, real_w], axis=-1),
                ],
                axis=0,
            )
            out[q] = jnp.dot(delayed, steer, preferred_element_type=jnp.float32).astype(out.dtype)


def work(jobs, dtypes, rows, count, length, height, width, **arrays):
    names = tuple(arrays)
    shapes = [pltpu.VMEM((rows, length, width), dtype) for dtype in dtypes]
    filters = sum(what == FILTER for what, _, _ in jobs)
    if filters:
        lanes = (height + 127) // 128 * 128
        shapes.append(pltpu.VMEM((filters, rows, length, lanes), jnp.bfloat16))
    flops = 0
    for what, _, _ in jobs:
        flops += 2 * rows * length * height * (
            (0 if what == STEER else length) + (0 if what == FILTER else width)
        )
    return pl.pallas_call(
        functools.partial(work_kernel, jobs, count, rows, names),
        out_shape=tuple(shapes),
        in_specs=[SMEM if name == "sets" else VMEM for name in names],
        out_specs=(VMEM,) * len(shapes),
        cost_estimate=pl.CostEstimate(flops=flops, bytes_accessed=flops // 256, transcendentals=0),
        compiler_params=PARAMS,
        name="work",
    )(*[near(value, pltpu.SMEM if name == "sets" else pltpu.VMEM) for name, value in arrays.items()])


def finish_kernel(right_ref, left_ref, own_ref, out_ref):
    rows, _, width = own_ref.shape
    half = width // 2
    for q in range(rows):
        total = (
            right_ref[q].astype(jnp.float32) + left_ref[q].astype(jnp.float32) + own_ref[q]
        )
        for part in range(2):
            out_ref[q, part] = total[:, part * half : (part + 1) * half].T.astype(out_ref.dtype)


def finish(right, left, own):
    rows, length, width = own.shape
    return pl.pallas_call(
        finish_kernel,
        out_shape=jax.ShapeDtypeStruct((rows, 2, width // 2, length), jnp.bfloat16),
        in_specs=[VMEM] * 3,
        out_specs=VMEM,
        compiler_params=PARAMS,
        name="finish",
    )(near(right), near(left), near(own))


def ring(voltages, delays, tap_sets, tap_table, weights):
    _, channels, pair, antennas, length = voltages.shape
    beam_count = weights.shape[-1]
    count = lax.axis_size("station")
    rows = channels // count
    half = count // 2
    height = pair * antennas
    x = voltages.reshape(count, rows, height, length)
    w = weights.reshape(count, rows, pair, antennas, beam_count)
    sizes = (rows, count, length, height, 2 * beam_count)
    wide, thin = jnp.float32, jnp.bfloat16

    pieces = [[half, half - 1, 1 - half]]
    pieces.append([o for s in (2, 3) for o in (half - s, s - half)])
    pieces.append([o for s in range(4, half) for o in (half - s, s - half)] + [0])
    halos = {}

    def use_piece(i, got, after=()):
        if after:
            got = settle(got, after)
        halos.update({o: (got, place) for place, o in enumerate(pieces[i])})

    packed = pack(x, pieces[0], False)
    use_piece(0, from_earlier(packed))
    main, edge, near_x, packed = bank(tap_table, delays, x, pieces[1])
    other_w = across_cores(w)
    second = packed
    common = {"sets": tap_sets, "main": main, "edge": edge, "x": near_x, "w": w}

    def filtered(offsets):
        jobs = tuple((FILTER, o, halos[o][1]) for o in offsets)
        return work(jobs, [], *sizes, **common, halo=halos[offsets[0]][0])[0]

    halo, place = halos[half]
    a, handed = work(
        ((BOTH, half, place), (FILTER, 1 - half, halos[1 - half][1])), [thin],
        *sizes, **common, halo=halo,
    )
    a_got = onward(a)
    given = {1: (across_cores(handed), 0)}
    halo, place = halos[half - 1]
    (own,) = work(((BOTH, half - 1, place),), [wide], *sizes, **common, halo=halo)
    second = from_earlier(second)
    packed = pack(near_x, pieces[2], True)
    (b,) = work(
        ((STEER, half - 1, 0),), [thin], *sizes, given=given[1][0], other_w=other_w
    )

    def send_filtered(first, last):
        over = filtered([s - half for s in range(first, last)])
        got = across_cores(over)
        got = settle(got)
        given.update({s: (got, s - first) for s in range(first, last)})

    for s in range(1, half):
        b_got = onward(b)
        a = (a_got.astype(wide) + own).astype(thin)
        a_got = onward(a)
        if s == 1:
            use_piece(1, second, (a, b))
            send_filtered(2, 4)
            third = from_earlier(packed)
        elif s == 3:
            use_piece(2, third, (a, b))
            send_filtered(4, half)
        halo, place = halos[half - s - 1]
        if s == half - 1:
            (own,) = work(((BOTH, 0, place),), [wide], *sizes, **common, halo=halo)
            break
        job = (BOTH, half - s - 1, place)
        if s != 3:
            own, other = work(
                (job, (STEER, half - s - 1, given[s + 1][1])), [wide, wide], *sizes, **common,
                halo=halo, given=given[s + 1][0], other_w=other_w,
            )
        else:
            (own,) = work((job,), [wide], *sizes, **common, halo=halo)
            (other,) = work(
                ((STEER, half - s - 1, given[s + 1][1]),), [wide], *sizes,
                given=given[s + 1][0], other_w=other_w,
            )
        b = (b_got.astype(wide) + other).astype(thin)
    back = across_cores(b_got)
    return finish(a_got, back, own)


def solution(mesh):
    return jax.shard_map(
        ring,
        mesh=mesh,
        in_specs=(
            P(("group", "station"), "chan", None, None, "tm"),
            P(("group", "station")),
            P(("group", "station"), "chan"),
            P(),
            P(("group", "station"), "chan", None, None, None),
        ),
        out_specs=P(("group", "chan", "station"), None, None, "tm"),
        check_vma=False,
    )
```
